256 devices in a mesh: row: 16 (over x, y), col: 16 (over z, core).
Axes of the slice: x: 4, y: 4, z: 8, core: 2. Of those that a mesh axis runs over, the one named last changes fastest.
Arguments:
- inputs: bfloat16 [2048, 16384], P('col', 'row'), may hold values from -6 to 6
- weight: bfloat16 [16384, 16384], P('row', 'col'), may hold values from -0.046875 to 0.046875
- cotangent: bfloat16 [2048, 16384], P('row', 'col'), may hold values from -0.75 to 0.75
- scale_in: float32 [8, 16384], P(None, 'row'), may hold values from -4 to 4
- scale_out: float32 [8, 16384], P(None, 'col'), may hold values from -4 to 4
- member: int32 [2048], replicated, may hold values from 0 to 7
Outputs:
- input_grad: bfloat16 [2048, 16384], P('col', 'row')
- weight_grad: float32 [16384, 16384], P('row', 'col')
- in_factor_grad: float32 [8, 16384], P(None, 'row')
- out_factor_grad: float32 [8, 16384], P(None, 'col')
The draws below stay inside these ranges and needn't reach their ends.
All inputs are finite; a program needn't handle non-finite values.
Results may differ from the reference program's by a relative error of at most 0.0049.
Values may be sent and summed in bfloat16 or wider, within the bound.
No kernel may reach another device: no remote copies, remote signals or barrier semaphores. Data moves between devices by JAX's collectives and lax.ppermute only.
A program may use at most 128 MiB of HBM per device.

```python
import jax
import jax.numpy as jnp

D = 16384
F = 16384
M = 8
BATCH = 2048


def place_ends(result, rng, low, high):
    spot = [jax.random.randint(jax.random.fold_in(rng, axis), (), 0, length) for axis, length in enumerate(result.shape)]
    main_axis = result.shape.index(max(result.shape))
    next_to = spot[:main_axis] + [(spot[main_axis] + 1) % result.shape[main_axis]] + spot[main_axis + 1:]
    return result.at[tuple(spot)].set(low).at[tuple(next_to)].set(high)


def shard_levels(own_key, extent, shards, low, high):
    level, own = 1.0, jax.random.fold_in(own_key, 6)
    for position, blocks in shards:
        draws = jnp.exp(jax.random.uniform(jax.random.fold_in(own, position), (blocks,), jnp.float32, low / len(shards), high / len(shards)))
        level = level * jnp.repeat(draws, extent[position] // blocks).reshape([-1 if axis == position else 1 for axis in range(len(extent))])
    return level


def scatter_about(stream_key, dims, deviation, reach, pieces=(), held_as=jnp.bfloat16):
    gain = shard_levels(stream_key, dims, pieces, -0.22, 0.18) if pieces else 1.0
    values = jax.random.normal(stream_key, dims, jnp.float32) * deviation * gain
    return jnp.minimum(jnp.maximum(values, -reach), reach).astype(held_as)


def setup_inputs(seed: int = 0) -> dict:
    streams_of = jax.random.split(jax.random.key(seed), 7)
    return {
        "inputs": scatter_about(streams_of[0], (BATCH, D), 1.0, 6.0, ((0, 16), (1, 16))),
        "weight": scatter_about(streams_of[1], (D, F), D ** -0.5, 0.046875, ((0, 16), (1, 16))),
        "cotangent": scatter_about(streams_of[2], (BATCH, F), 0.125, 0.75, ((0, 16), (1, 16))),
        "scale_in": scatter_about(streams_of[3], (M, D), 1.0, 4.0, ((1, 16),), jnp.float32),
        "scale_out": scatter_about(streams_of[4], (M, F), 1.0, 4.0, ((1, 16),), jnp.float32),
        "member": place_ends(jax.random.randint(streams_of[5], (BATCH,), 0, M), jax.random.fold_in(streams_of[5], 1), 0, M - 1).astype(jnp.int32),
    }


def reference(inputs, weight, cotangent, scale_in, scale_out, member):
    r_rows = scale_in[member]
    s_rows = scale_out[member]
    scaled_in = (inputs.astype(jnp.float32) * r_rows).astype(jnp.bfloat16)
    scaled_cot = (cotangent.astype(jnp.float32) * s_rows).astype(jnp.bfloat16)
    pre_out = jnp.dot(scaled_in, weight, preferred_element_type=jnp.float32)
    out_factor_grad = jax.ops.segment_sum(cotangent.astype(jnp.float32) * pre_out, member, num_segments=M)
    back_in = jnp.dot(scaled_cot, weight.T, preferred_element_type=jnp.float32)
    input_grad = (back_in * r_rows).astype(jnp.bfloat16)
    in_factor_grad = jax.ops.segment_sum(inputs.astype(jnp.float32) * back_in, member, num_segments=M)
    weight_grad = jnp.dot(scaled_in.T, scaled_cot, preferred_element_type=jnp.float32)
    return input_grad, weight_grad, in_factor_grad, out_factor_grad
```

```python
import functools

import jax
import jax.numpy as jnp
from jax import lax
from jax.experimental import pallas as pl
from jax.experimental.pallas import tpu as pltpu
from jax.sharding import Mesh, PartitionSpec as P


NX, NY, NZ = 4, 4, 8
F32, BF16 = jnp.float32, jnp.bfloat16
PLANE = (0, -1, 1, 2)


def ring(n, d):
    return [(i, (i + d) % n) for i in range(n)]


def shift(value, axis, n, d):
    return lax.ppermute(value, axis, ring(n, d))


def flip(value, axis, n, bit):
    return lax.ppermute(value, axis, [(i, i ^ bit) for i in range(n)])


def dot(a, b):
    return jnp.dot(a, b, preferred_element_type=F32)


def summed(hot_t, values):
    high = values.astype(BF16)
    low = (values - high.astype(F32)).astype(BF16)
    return dot(hot_t, high) + dot(hot_t, low)


def join_kernel(*refs):
    for n, out in enumerate(refs[8:]):
        for m, part in enumerate(refs[4 * n : 4 * n + 4]):
            out[m * 64 : m * 64 + 64, :] = part[...]


def turn_kernel(weight, weight_t):
    for n in range(4):
        part = slice(n * 256, n * 256 + 256)
        weight_t[:, part] = weight[part, :].T


def back_kernel(fars, at, hot, factors, weight_t, *refs):
    stacks, (cot_all, scaled_all, own_other) = refs[: 2 * len(fars)], refs[-3:]
    x, y, z, c = at[0], at[1], at[2], at[3]
    for n, stack in enumerate(stacks):
        far, turned = fars[n // 2], n % 2
        starts, places = [], []
        for d in PLANE:
            i, j = (far, d) if turned else (d, far)
            i, j = lax.rem(x + i + 4, 4), lax.rem(y + j + 4, 4)
            near = lax.rem(i * 2 + lax.div(j, 2) - z + 8, 8)
            side = lax.rem(j + c, 2)
            part = turned * 64
            starts.append(pl.multiple_of((near * 2 + side) * 128 + part, 64))
            places.append(pl.multiple_of((side * 8 + near) * 128 + part, 64))
        hots = jnp.concatenate([hot[pl.ds(s, 64), :] for s in starts], 0)
        values = stack[...]
        scaled = (values.astype(F32) * dot(hots, factors[...])).astype(BF16)
        back = dot(scaled, weight_t[...]).astype(BF16)
        for p in range(4):
            rows = slice(p * 64, p * 64 + 64)
            cot_all[pl.ds(starts[p], 64), :] = values[rows]
            scaled_all[pl.ds(starts[p], 64), :] = scaled[rows]
            own_other[pl.ds(places[p], 64), :] = back[rows]


def paired(refs, n):
    parts = []
    for m in (2 * n, 2 * n + 1):
        for piece in refs[m], refs[8 + m]:
            parts += [p[...] for p in piece]
    return jnp.concatenate(parts, 0)


def pieces(refs):
    return [
        [r] for r in refs[:4]] + [list(refs[4:6])] + [[r] for r in refs[6:9]]


def in_kernel(hot_t, back, *refs):
    in_term, held = refs[-1], pieces(refs[:9]) + pieces(refs[9:18])
    for n in range(4):
        near = [
            back[k * 128 : k * 128 + 128, :] for m in (2 * n, 2 * n + 1) for k in (m, 8 + m)
        ]
        values = paired(held, n).astype(F32) * jnp.concatenate(near, 0).astype(F32)
        term = summed(hot_t[:, n * 512 : n * 512 + 512], values)
        in_term[...] = term if n == 0 else in_term[...] + term


def front_kernel(first, hot, hot_t, factors, weight, cot_all, *refs):
    (scaled_all, out_term), held = refs[-2:], pieces(refs[:9]) + pieces(refs[9:18])
    for n in range(2):
        own = slice(n * 512, n * 512 + 512)
        part = slice(first + n * 512, first + n * 512 + 512)
        values = paired(held, first // 512 + n).astype(F32)
        scaled = (values * dot(hot[part, :], factors[...])).astype(BF16)
        scaled_all[own, :] = scaled
        product = cot_all[part, :].astype(F32) * dot(scaled, weight[...])
        term = summed(hot_t[:, part], product)
        out_term[...] = term if n == 0 else out_term[...] + term


def grad_kernel(first, second, scaled_cot, *refs):
    half, grad = scaled_cot.shape[0] // 2, refs[-1]
    grad[...] = sum(
        lax.dot_general(
            part[...],
            scaled_cot[n * half : n * half + half, :],
            (((0,), (0,)), ((), ())),
            preferred_element_type=F32,
        )
        for n, part in enumerate((first, second))
    )


def grad_part(first, second, scaled_cot, n, before=()):
    tile = pl.BlockSpec((1024, 256), lambda i: (0, i + 2 * n))
    return pl.pallas_call(
        grad_kernel,
        grid=(2,),
        out_shape=jax.ShapeDtypeStruct((1024, 1024), F32),
        in_specs=[tile, tile, pl.BlockSpec(memory_space=pltpu.VMEM)]
        + [pl.BlockSpec(memory_space=pl.ANY)] * len(before),
        out_specs=pl.BlockSpec((256, 1024), lambda i: (i + 2 * n, 0)),
        input_output_aliases={3: 0} if before else {},
        compiler_params=pltpu.CompilerParams(vmem_limit_bytes=24 * 2**20),
    )(first, second, scaled_cot, *before)


def call(kernel, outs, limit, *args, smem=0, aliases={}):
    vmem = pl.BlockSpec(memory_space=pltpu.VMEM)
    return pl.pallas_call(
        kernel,
        out_shape=[jax.ShapeDtypeStruct(*o) for o in outs],
        in_specs=[pl.BlockSpec(memory_space=pltpu.SMEM)] * smem + [vmem] * (len(args) - smem),
        out_specs=[vmem] * len(outs),
        input_output_aliases=aliases,
        compiler_params=pltpu.CompilerParams(vmem_limit_bytes=limit * 2**20),
    )(*args)


def thirds(factors):
    def cut(value):
        return lax.reduce_precision(value, 8, 7)

    high = cut(factors)
    middle = cut(factors - high)
    low = factors - high - middle
    parts = jnp.concatenate([high, middle, low], 0).astype(BF16)
    return jnp.pad(parts, ((0, 128 - parts.shape[0]), (0, 0)))


def step(inputs, weight, cotangent, scale_in, scale_out, member):
    a, b = cotangent[:64], cotangent[64:]
    a4 = [a] + [shift(a, "x", NX, -d) for d in PLANE[1:]]
    b4 = [b] + [shift(b, "y", NY, -d) for d in PLANE[1:]]
    stack = ((256, 1024), BF16)
    a4, b4 = call(join_kernel, [stack, stack], 8, *a4, *b4)
    (weight_t,) = call(turn_kernel, [((1024, 1024), BF16)], 16, weight)
    a4, b4, member, scale_in, scale_out = lax.optimization_barrier(
        (a4, b4, member, scale_in, scale_out)
    )
    a_stacks = [a4] + [shift(a4, "y", NY, -d) for d in PLANE[1:]]
    b_stacks = [b4] + [shift(b4, "x", NX, -d) for d in PLANE[1:]]

    at = jnp.stack([lax.axis_index(a) for a in ("x", "y", "z", "c")]).astype(jnp.int32)
    blocks = member.reshape(NZ, 2, 128)
    blocks = lax.dynamic_slice_in_dim(jnp.concatenate([blocks, blocks], 0), at[2], NZ, 0)
    near = jnp.where(at[3] == 0, blocks, blocks[:, ::-1]).reshape(-1)
    ids = jnp.arange(128, dtype=jnp.int32)
    hot = ((near[:, None] == (ids % 8)[None, :]) & (ids < 24)[None, :]).astype(BF16)
    hot_t = (near[None, :] == jnp.arange(16, dtype=jnp.int32)[:, None]).astype(BF16)
    s3, r3 = thirds(scale_out), thirds(scale_in)

    up = down = inputs
    before, after = [], []
    for _ in range(3):
        up = shift(up, "z", NZ, 1)
        down = shift(down, "z", NZ, -1)
        before, after = [up] + before, after + [down]
    far = [shift(up[:64], "z", NZ, 1), shift(down[64:], "z", NZ, -1)]
    held = [inputs] + after + far + before
    held += [flip(h, "c", 2, 1) for h in held]

    whole, half, term = ((2048, 1024), BF16), ((1024, 1024), BF16), ((16, 1024), F32)
    filled = ()
    for n, (fars, which) in enumerate(((PLANE[:1], (0,)), (PLANE[1:3], (1, 2)), (PLANE[3:], (3,)))):
        stacks = [t for k in which for t in (a_stacks[k], b_stacks[k])]
        filled = call(
            functools.partial(back_kernel, fars), [whole, whole, whole], 32,
            at, hot, s3, weight_t, *stacks, *filled, smem=1,
            aliases={4 + len(stacks) + k: k for k in range(3)} if n else {},
        )
    cot_all, scaled_cot, back = filled
    own = back[:1024]
    theirs = flip(back[1024:], "c", 2, 1)
    (in_term,) = call(in_kernel, [term], 24, hot_t, back, *held)

    def step_sum(n, arrived, rows=slice(0, 128)):
        arrived, ours, others = lax.optimization_barrier((arrived, own, theirs))
        first = (n % 8) * 128
        part = slice(first + rows.start, first + rows.stop)
        total = ours[part].astype(F32) + others[part].astype(F32)
        return (total + arrived.astype(F32)).astype(BF16)

    nothing = jnp.zeros((64, 1024), BF16)
    right = shift(step_sum(4, nothing, slice(0, 64)), "z", NZ, 1)
    left = shift(step_sum(4, nothing, slice(64, 128)), "z", NZ, -1)
    right, left = jnp.concatenate([right, nothing], 0), jnp.concatenate([nothing, left], 0)
    for n in (3, 2, 1):
        right = shift(step_sum(n, right), "z", NZ, 1)
        left = shift(step_sum(-n, left), "z", NZ, -1)
    back_block = own[:128].astype(F32) + theirs[:128].astype(F32)
    back_block = back_block + right.astype(F32) + left.astype(F32)
    input_grad = (back_block * dot(hot[:128], r3)).astype(BF16)

    out_term, scaled_in = 0, []
    for n in range(2):
        scaled, part = call(
            functools.partial(front_kernel, n * 1024), [half, term], 24,
            hot, hot_t, r3, weight, cot_all, *held,
        )
        scaled_in.append(scaled)
        out_term = out_term + part[:8]
    weight_grad = grad_part(*scaled_in, scaled_cot, 0)
    weight_grad = grad_part(*scaled_in, scaled_cot, 1, (weight_grad,))
    in_term = in_term[:8]
    in_term = in_term + flip(in_term, "c", 2, 1)
    for bit in (1, 2, 4):
        in_term = in_term + flip(in_term, "z", NZ, bit)
    for axis, bit in (("x", 1), ("y", 1), ("x", 2), ("y", 2)):
        out_term = out_term + flip(out_term, axis, 4, bit)
    return (input_grad, weight_grad, in_term, out_term)


def solution(mesh):
    fine = Mesh(mesh.devices.reshape(NX, NY, NZ, 2), ("x", "y", "z", "c"))
    row, col = ("x", "y"), ("z", "c")
    return jax.shard_map(
        step,
        mesh=fine,
        in_specs=(P(col, row), P(row, col), P(row, col), P(None, row), P(None, col), P()),
        out_specs=(P(col, row), P(row, col), P(None, row), P(None, col)),
        check_vma=False,
    )
```

```python
import functools

import jax
import jax.numpy as jnp
from jax import lax
from jax.experimental import pallas as pl
from jax.experimental.pallas import tpu as pltpu
from jax.sharding import Mesh, PartitionSpec as P


NX, NY, NZ = 4, 4, 8
F32, BF16 = jnp.float32, jnp.bfloat16
PLANE = (0, -1, 1, 2)
LINE = (0, 1, 2, 6, 7, 3, 4, 5)
NEAR = 5


def ring(n, d):
    return [(i, (i + d) % n) for i in range(n)]


def shift(value, axis, n, d):
    return lax.ppermute(value, axis, ring(n, d))


def flip(value, axis, n, bit):
    return lax.ppermute(value, axis, [(i, i ^ bit) for i in range(n)])


def dot(a, b):
    return jnp.dot(a, b, preferred_element_type=F32)


def summed(hot_t, values):
    return dot(hot_t, values.astype(BF16))


def join_kernel(count, *refs):
    parts, outs = refs[:-count], refs[-count:]
    each = len(parts) // count
    for n, part in enumerate(parts):
        size = part.shape[0]
        outs[n // each][n % each * size : n % each * size + size, :] = part[...]


def stacks_kernel(*refs):
    for n in range(2):
        for m, part in enumerate(refs[4 * n : 4 * n + 4]):
            turned = (m + 2) % 4
            refs[8 + n][m * 64 : m * 64 + 64, :] = part[...]
            refs[10 + n][turned * 64 : turned * 64 + 64, :] = part[...]


def turn_kernel(weight, weight_t):
    for n in range(4):
        part = slice(n * 256, n * 256 + 256)
        weight_t[:, part] = weight[part, :].T


def back_kernel(fars, at, hot, factors, weight_t, *refs):
    stacks, (cot_all, scaled_all, own_other, pool) = refs[:-4], refs[-4:]
    x, y, z, c = at[0], at[1], at[2], at[3]
    row = 0
    for stack in stacks:
        if row < pool.shape[0]:
            pool[row : row + stack.shape[0], :] = stack[...]
            row += stack.shape[0]

    def stack_of(n, carry):
        turned = lax.rem(n, 2)
        far = fars[0]
        for m, other in enumerate(fars[1:]):
            far = jnp.where(n < 2 * m + 2, far, other)
        part = turned * 64
        starts, places = [], []
        for p, d in enumerate(PLANE):
            d = jnp.where(far == 1, PLANE[(p + 2) % 4], d)
            i = lax.rem(x + jnp.where(turned == 1, far, d) + 4, 4)
            j = lax.rem(y + jnp.where(turned == 1, d, far) + 4, 4)
            near = lax.rem(i * 2 + lax.div(j, 2) - z + 8, 8)
            spot = jnp.where(near < 3, near, jnp.where(near > 5, near - 3, near + 2))
            side = lax.rem(j + c, 2)
            starts.append(pl.multiple_of((spot * 2 + side) * 128 + part, 64))
            places.append(pl.multiple_of((side * 8 + spot) * 128 + part, 64))
        hots = jnp.concatenate([hot[pl.ds(s, 64), :] for s in starts], 0)
        values = pool[both(n), :]
        scaled = (values.astype(F32) * dot(hots, factors[...])).astype(BF16)
        back = dot(scaled, weight_t[...]).astype(BF16)
        for p in range(4):
            rows = slice(p * 64, p * 64 + 64)
            cot_all[pl.ds(starts[p], 64), :] = values[rows]
            scaled_all[pl.ds(starts[p], 64), :] = scaled[rows]
            own_other[pl.ds(places[p], 64), :] = back[rows]
        return carry

    lax.fori_loop(0, 2 * len(fars), stack_of, 0)


def block(n):
    return pl.ds(pl.multiple_of(n * 128, 128), 128)


def both(n):
    return pl.ds(pl.multiple_of(n * 256, 256), 256)


def in_kernel(hot_t, back, *refs):
    in_term = refs[-1]
    in_term[...] = jnp.zeros_like(in_term)
    for first, last, own, other in ((0, NEAR, *refs[:2]), (NEAR, NZ, *refs[2:4])):

        def chip(n, carry):
            values = jnp.concatenate([own[block(n - first), :], other[block(n - first), :]], 0)
            sums = jnp.concatenate([back[block(n), :], back[block(8 + n), :]], 0)
            in_term[...] += summed(hot_t[:, both(n)], values.astype(F32) * sums.astype(F32))
            return carry

        lax.fori_loop(first, last, chip, 0)


def front_kernel(first, hot, hot_t, factors, weight, cot_all, own, other, before, *outs):
    scaled_all, out_term = outs
    out_term[...] = before[...]

    def chip(n, carry):
        rows = both(first + n)
        values = jnp.concatenate([own[block(n), :], other[block(n), :]], 0).astype(F32)
        scaled = (values * dot(hot[rows, :], factors[...])).astype(BF16)
        scaled_all[both(n), :] = scaled
        product = cot_all[rows, :].astype(F32) * dot(scaled, weight[...])
        out_term[...] += summed(hot_t[:, rows], product)
        return carry

    lax.fori_loop(0, own.shape[0] // 128, chip, 0)


def grad_kernel(first, second, scaled_cot, *refs):
    split, grad = first.shape[0], refs[-1]
    grad[...] = sum(
        lax.dot_general(part[...], rows, (((0,), (0,)), ((), ())), preferred_element_type=F32)
        for part, rows in ((first, scaled_cot[:split, :]), (second, scaled_cot[split:, :]))
    )


def grad_part(first, second, scaled_cot, n, before=()):
    tiles = [pl.BlockSpec((p.shape[0], 256), lambda i: (0, i + 2 * n)) for p in (first, second)]
    return pl.pallas_call(
        grad_kernel,
        grid=(2,),
        out_shape=jax.ShapeDtypeStruct((1024, 1024), F32),
        in_specs=tiles
        + [pl.BlockSpec(memory_space=pltpu.VMEM)]
        + [pl.BlockSpec(memory_space=pl.ANY)] * len(before),
        out_specs=pl.BlockSpec((256, 1024), lambda i: (i + 2 * n, 0)),
        input_output_aliases={3: 0} if before else {},
        compiler_params=pltpu.CompilerParams(vmem_limit_bytes=16 * 2**20),
    )(first, second, scaled_cot, *before)


def call(kernel, outs, limit, *args, smem=0, aliases={}, scratch=()):
    vmem = pl.BlockSpec(memory_space=pltpu.VMEM)
    return pl.pallas_call(
        kernel,
        out_shape=[jax.ShapeDtypeStruct(*o) for o in outs],
        in_specs=[pl.BlockSpec(memory_space=pltpu.SMEM)] * smem + [vmem] * (len(args) - smem),
        out_specs=[vmem] * len(outs),
        input_output_aliases=aliases,
        scratch_shapes=scratch,
        compiler_params=pltpu.CompilerParams(vmem_limit_bytes=limit * 2**20),
    )(*args)


def thirds(factors):
    def cut(value):
        return lax.reduce_precision(value, 8, 7)

    high = cut(factors)
    middle = cut(factors - high)
    low = factors - high - middle
    parts = jnp.concatenate([high, middle, low], 0).astype(BF16)
    return jnp.pad(parts, ((0, 128 - parts.shape[0]), (0, 0)))


def step(inputs, weight, cotangent, scale_in, scale_out, member):
    a, b = cotangent[:64], cotangent[64:]
    a4 = [a] + [shift(a, "x", NX, -d) for d in PLANE[1:]]
    b4 = [b] + [shift(b, "y", NY, -d) for d in PLANE[1:]]
    stack = ((256, 1024), BF16)
    a4, b4, a4_back, b4_back = call(stacks_kernel, [stack] * 4, 8, *a4, *b4)
    (weight_t,) = call(turn_kernel, [((1024, 1024), BF16)], 8, weight)
    a4, b4, member, scale_in, scale_out = lax.optimization_barrier(
        (a4, b4, member, scale_in, scale_out)
    )

    def around(own, own_back, axis):
        before = shift(own, axis, 4, 1)
        after = shift(own_back, axis, 4, -1)
        far = (shift(before[:128], axis, 4, 1), shift(after[:128], axis, 4, -1))
        return before, after, far

    a_stacks, b_stacks = around(a4, a4_back, "y"), around(b4, b4_back, "x")

    at = jnp.stack([lax.axis_index(a) for a in ("x", "y", "z", "c")]).astype(jnp.int32)
    blocks = member.reshape(NZ, 2, 128)
    blocks = lax.dynamic_slice_in_dim(jnp.concatenate([blocks, blocks], 0), at[2], NZ, 0)
    blocks = jnp.where(at[3] == 0, blocks, blocks[:, ::-1])
    near = jnp.concatenate([blocks[:3], blocks[6:], blocks[3:6]], 0).reshape(-1)
    ids = jnp.arange(128, dtype=jnp.int32)
    hot = ((near[:, None] == (ids % 8)[None, :]) & (ids < 24)[None, :]).astype(BF16)
    hot_t = (near[None, :] == jnp.arange(16, dtype=jnp.int32)[:, None]).astype(BF16)
    s3, r3 = thirds(scale_out), thirds(scale_in)

    ups, downs = [inputs], [inputs]
    for _ in range(3):
        ups.append(shift(ups[-1], "z", NZ, 1))
        downs.append(shift(downs[-1], "z", NZ, -1))
    downs.append(shift(downs[-1], "z", NZ, -1))
    near_set = [inputs, downs[1], downs[2], ups[2], ups[1]]
    join = functools.partial(join_kernel, 1)
    (x_near,) = call(join, [((NEAR * 128, 1024), BF16)], 8, *near_set)
    (x_far,) = call(join, [((1024 - NEAR * 128, 1024), BF16)], 8, downs[3], downs[4], ups[3])
    held = [x_near, flip(x_near, "c", 2, 1), x_far, flip(x_far, "c", 2, 1)]

    whole, term = ((2048, 1024), BF16), ((16, 1024), F32)
    filled = ()
    for n, (fars, stacks) in enumerate((
        (PLANE[:1], (a4, b4)),
        (PLANE[1:3], (a_stacks[0], b_stacks[0], a_stacks[1], b_stacks[1])),
        (PLANE[3:], (*a_stacks[2], *b_stacks[2])),
    )):
        filled = call(
            functools.partial(back_kernel, fars), [whole, whole, whole], 12,
            at, hot, s3, weight_t, *stacks, *filled, smem=1,
            aliases={4 + len(stacks) + k: k for k in range(3)} if n else {},
            scratch=[pltpu.VMEM((len(fars) * 512, 1024), BF16)],
        )
    cot_all, scaled_cot, back = filled
    own = back[:1024]
    theirs = flip(back[1024:], "c", 2, 1)
    (in_term,) = call(in_kernel, [term], 8, hot_t, back, *held)

    def step_sum(n, arrived=None):
        first = LINE.index(n % 8) * 128
        part = slice(first, first + 128)
        if arrived is None:
            return (own[part].astype(F32) + theirs[part].astype(F32)).astype(BF16)
        arrived, ours, others = lax.optimization_barrier((arrived, own, theirs))
        total = ours[part].astype(F32) + others[part].astype(F32)
        return (total + arrived.astype(F32)).astype(BF16)

    right = shift(step_sum(4), "z", NZ, 1)
    left = shift(step_sum(-3), "z", NZ, -1)
    for n in (3, 2, 1):
        right = shift(step_sum(n, right), "z", NZ, 1)
        if n > 1:
            left = shift(step_sum(1 - n, left), "z", NZ, -1)
    back_block = own[:128].astype(F32) + theirs[:128].astype(F32)
    back_block = back_block + right.astype(F32) + left.astype(F32)
    input_grad = (back_block * dot(hot[:128], r3)).astype(BF16)

    out_term, scaled_in = jnp.zeros((16, 1024), F32), []
    for n, first in enumerate((0, NEAR)):
        parts = held[2 * n : 2 * n + 2]
        scaled, out_term = call(
            functools.partial(front_kernel, first),
            [((parts[0].shape[0] * 2, 1024), BF16), term], 10,
            hot, hot_t, r3, weight, cot_all, *parts, out_term,
        )
        scaled_in.append(scaled)
    weight_grad = grad_part(*scaled_in, scaled_cot, 0)
    weight_grad = grad_part(*scaled_in, scaled_cot, 1, (weight_grad,))
    in_term, out_term = in_term[:8], out_term[:8]
    in_term = in_term + flip(in_term, "c", 2, 1)
    for bit in (1, 2, 4):
        in_term = in_term + flip(in_term, "z", NZ, bit)
    for axis, bit in (("x", 1), ("y", 1), ("x", 2), ("y", 2)):
        out_term = out_term + flip(out_term, axis, 4, bit)
    return (input_grad, weight_grad, in_term, out_term)


def solution(mesh):
    fine = Mesh(mesh.devices.reshape(NX, NY, NZ, 2), ("x", "y", "z", "c"))
    row, col = ("x", "y"), ("z", "c")
    return jax.shard_map(
        step,
        mesh=fine,
        in_specs=(P(col, row), P(row, col), P(row, col), P(None, row), P(None, col), P()),
        out_specs=(P(col, row), P(row, col), P(None, row), P(None, col)),
        check_vma=False,
    )
```

```python
import functools

import jax
import jax.numpy as jnp
from jax import lax
from jax.experimental import pallas as pl
from jax.experimental.pallas import tpu as pltpu
from jax.sharding import Mesh, PartitionSpec as P


NX, NY, NZ = 4, 4, 8
F32, BF16 = jnp.float32, jnp.bfloat16
PLANE = (0, -1, 1, 2)
LINE = (0, 1, 2, 6, 7, 3, 4, 5)
NEAR = 5


def ring(n, d):
    return [(i, (i + d) % n) for i in range(n)]


def shift(value, axis, n, d):
    return lax.ppermute(value, axis, ring(n, d))


def flip(value, axis, n, bit):
    return lax.ppermute(value, axis, [(i, i ^ bit) for i in range(n)])


def dot(a, b):
    return jnp.dot(a, b, preferred_element_type=F32)


def summed(hot_t, values):
    return dot(hot_t, values.astype(BF16))


def join_kernel(count, *refs):
    parts, outs = refs[:-count], refs[-count:]
    each = len(parts) // count
    for n, part in enumerate(parts):
        size = part.shape[0]
        outs[n // each][n % each * size : n % each * size + size, :] = part[...]


def stacks_kernel(*refs):
    for n in range(2):
        for m, part in enumerate(refs[4 * n : 4 * n + 4]):
            turned = (m + 2) % 4
            refs[8 + n][m * 64 : m * 64 + 64, :] = part[...]
            refs[10 + n][turned * 64 : turned * 64 + 64, :] = part[...]


def turn_kernel(at, member, scale_in, scale_out, weight, weight_t, hot, hot_t, r3, s3):
    for n in range(4):
        part = slice(n * 256, n * 256 + 256)
        weight_t[:, part] = weight[part, :].T
    z, c = at[2], at[3]
    ids = lax.broadcasted_iota(jnp.int32, (128, 128), 0)
    for n, near in enumerate(LINE):
        for side in range(2):
            k = lax.rem(z + near, 8) * 2 + lax.rem(side + c, 2)
            here = jnp.broadcast_to(member[pl.ds(k, 1), :], (128, 128))
            part = slice((2 * n + side) * 128, (2 * n + side) * 128 + 128)
            match = jnp.where((here == lax.rem(ids, 8)) & (ids < 24), 1.0, 0.0)
            hot[part, :] = match.T.astype(BF16)
            hot_t[:, part] = jnp.where(here[:16] == ids[:16], 1.0, 0.0).astype(BF16)
    for factors, out in ((scale_in, r3), (scale_out, s3)):
        value = factors[...]
        high = value.astype(BF16).astype(F32)
        middle = (value - high).astype(BF16).astype(F32)
        parts = [high, middle, value - high - middle, jnp.zeros((104, 1024), F32)]
        out[...] = jnp.concatenate(parts, 0).astype(BF16)


def back_kernel(fars, at, hot, factors, weight_t, *refs):
    stacks, (cot_all, scaled_all, own_other, pool) = refs[:-4], refs[-4:]
    x, y, z, c = at[0], at[1], at[2], at[3]
    row = 0
    for stack in stacks:
        if row < pool.shape[0]:
            pool[row : row + stack.shape[0], :] = stack[...]
            row += stack.shape[0]

    def stack_of(n, carry):
        turned = lax.rem(n, 2)
        far = fars[0]
        for m, other in enumerate(fars[1:]):
            far = jnp.where(n < 2 * m + 2, far, other)
        part = turned * 64
        starts, places = [], []
        for p, d in enumerate(PLANE):
            d = jnp.where(far == 1, PLANE[(p + 2) % 4], d)
            i = lax.rem(x + jnp.where(turned == 1, far, d) + 4, 4)
            j = lax.rem(y + jnp.where(turned == 1, d, far) + 4, 4)
            near = lax.rem(i * 2 + lax.div(j, 2) - z + 8, 8)
            spot = jnp.where(near < 3, near, jnp.where(near > 5, near - 3, near + 2))
            side = lax.rem(j + c, 2)
            starts.append(pl.multiple_of((spot * 2 + side) * 128 + part, 64))
            places.append(pl.multiple_of((side * 8 + spot) * 128 + part, 64))
        hots = jnp.concatenate([hot[pl.ds(s, 64), :] for s in starts], 0)
        values = pool[both(n), :]
        scaled = (values.astype(F32) * dot(hots, factors[...])).astype(BF16)
        back = dot(scaled, weight_t[...]).astype(BF16)
        for p in range(4):
            rows = slice(p * 64, p * 64 + 64)
            cot_all[pl.ds(starts[p], 64), :] = values[rows]
            scaled_all[pl.ds(starts[p], 64), :] = scaled[rows]
            own_other[pl.ds(places[p], 64), :] = back[rows]
        return carry

    lax.fori_loop(0, 2 * len(fars), stack_of, 0)


def block(n):
    return pl.ds(pl.multiple_of(n * 128, 128), 128)


def both(n):
    return pl.ds(pl.multiple_of(n * 256, 256), 256)


def in_kernel(hot_t, back, *refs):
    in_term = refs[-1]
    in_term[...] = jnp.zeros_like(in_term)
    for first, last, own, other in ((0, NEAR, *refs[:2]), (NEAR, NZ, *refs[2:4])):

        def chip(n, carry):
            values = jnp.concatenate([own[block(n - first), :], other[block(n - first), :]], 0)
            sums = jnp.concatenate([back[block(n), :], back[block(8 + n), :]], 0)
            in_term[...] += summed(hot_t[:, both(n)], values.astype(F32) * sums.astype(F32))
            return carry

        lax.fori_loop(first, last, chip, 0)


def front_kernel(first, hot, hot_t, factors, weight, cot_all, own, other, before, *outs):
    scaled_all, out_term = outs
    out_term[...] = before[...]

    def chip(n, carry):
        rows = both(first + n)
        values = jnp.concatenate([own[block(n), :], other[block(n), :]], 0).astype(F32)
        scaled = (values * dot(hot[rows, :], factors[...])).astype(BF16)
        scaled_all[both(n), :] = scaled
        product = cot_all[rows, :].astype(F32) * dot(scaled, weight[...])
        out_term[...] += summed(hot_t[:, rows], product)
        return carry

    lax.fori_loop(0, own.shape[0] // 128, chip, 0)


def grad_kernel(first, second, scaled_cot, *refs):
    split, grad = first.shape[0], refs[-1]
    grad[...] = sum(
        lax.dot_general(part[...], rows, (((0,), (0,)), ((), ())), preferred_element_type=F32)
        for part, rows in ((first, scaled_cot[:split, :]), (second, scaled_cot[split:, :]))
    )


def grad_part(first, second, scaled_cot, n, before=()):
    tiles = [pl.BlockSpec((p.shape[0], 256), lambda i: (0, i + 2 * n)) for p in (first, second)]
    return pl.pallas_call(
        grad_kernel,
        grid=(2,),
        out_shape=jax.ShapeDtypeStruct((1024, 1024), F32),
        in_specs=tiles
        + [pl.BlockSpec(memory_space=pltpu.VMEM)]
        + [pl.BlockSpec(memory_space=pl.ANY)] * len(before),
        out_specs=pl.BlockSpec((256, 1024), lambda i: (i + 2 * n, 0)),
        input_output_aliases={3: 0} if before else {},
        compiler_params=pltpu.CompilerParams(vmem_limit_bytes=16 * 2**20),
    )(first, second, scaled_cot, *before)


def call(kernel, outs, limit, *args, smem=0, aliases={}, scratch=(), fetch=False):
    vmem = pl.BlockSpec(memory_space=pltpu.VMEM)
    ins = [pl.BlockSpec(a.shape, lambda i: (0, 0)) if fetch else vmem for a in args[smem:]]
    return pl.pallas_call(
        kernel,
        grid=(1,) if fetch else (),
        out_shape=[jax.ShapeDtypeStruct(*o) for o in outs],
        in_specs=[pl.BlockSpec(memory_space=pltpu.SMEM)] * smem + ins,
        out_specs=[vmem] * len(outs),
        input_output_aliases=aliases,
        scratch_shapes=scratch,
        compiler_params=pltpu.CompilerParams(vmem_limit_bytes=limit * 2**20),
    )(*args)


def step(inputs, weight, cotangent, scale_in, scale_out, member):
    a, b = cotangent[:64], cotangent[64:]
    a4 = [a] + [shift(a, "x", NX, -d) for d in PLANE[1:]]
    b4 = [b] + [shift(b, "y", NY, -d) for d in PLANE[1:]]
    stack = ((256, 1024), BF16)
    a4, b4, a4_back, b4_back = call(stacks_kernel, [stack] * 4, 8, *a4, *b4)
    at = jnp.stack([lax.axis_index(a) for a in ("x", "y", "z", "c")]).astype(jnp.int32)
    weight_t, hot, hot_t, r3, s3 = call(
        turn_kernel,
        [((1024, 1024), BF16), ((2048, 128), BF16), ((16, 2048), BF16)] + [((128, 1024), BF16)] * 2,
        12, at, member.reshape(16, 128), scale_in, scale_out, weight, smem=1,
        fetch=True,
    )

    def around(own, own_back, axis):
        before = shift(own, axis, 4, 1)
        after = shift(own_back, axis, 4, -1)
        far = (shift(before[:128], axis, 4, 1), shift(after[:128], axis, 4, -1))
        return before, after, far

    a_stacks, b_stacks = around(a4, a4_back, "y"), around(b4, b4_back, "x")

    ups, downs = [inputs], [inputs]
    for _ in range(3):
        ups.append(shift(ups[-1], "z", NZ, 1))
        downs.append(shift(downs[-1], "z", NZ, -1))
    downs.append(shift(downs[-1], "z", NZ, -1))
    near_set = [inputs, downs[1], downs[2], ups[2], ups[1]]
    join = functools.partial(join_kernel, 1)
    (x_near,) = call(join, [((NEAR * 128, 1024), BF16)], 8, *near_set)
    (x_far,) = call(join, [((1024 - NEAR * 128, 1024), BF16)], 8, downs[3], downs[4], ups[3])
    held = [x_near, flip(x_near, "c", 2, 1), x_far, flip(x_far, "c", 2, 1)]

    whole, term = ((2048, 1024), BF16), ((16, 1024), F32)
    filled = ()
    for n, (fars, stacks) in enumerate((
        (PLANE[:1], (a4, b4)),
        (PLANE[1:3], (a_stacks[0], b_stacks[0], a_stacks[1], b_stacks[1])),
        (PLANE[3:], (*a_stacks[2], *b_stacks[2])),
    )):
        filled = call(
            functools.partial(back_kernel, fars), [whole, whole, whole], 12,
            at, hot, s3, weight_t, *stacks, *filled, smem=1,
            aliases={4 + len(stacks) + k: k for k in range(3)} if n else {},
            scratch=[pltpu.VMEM((len(fars) * 512, 1024), BF16)],
        )
    cot_all, scaled_cot, back = filled
    own = back[:1024]
    theirs = flip(back[1024:], "c", 2, 1)
    (in_term,) = call(in_kernel, [term], 8, hot_t, back, *held)

    def step_sum(n, arrived=None):
        first = LINE.index(n % 8) * 128
        part = slice(first, first + 128)
        if arrived is None:
            return (own[part].astype(F32) + theirs[part].astype(F32)).astype(BF16)
        arrived, ours, others = lax.optimization_barrier((arrived, own, theirs))
        total = ours[part].astype(F32) + others[part].astype(F32)
        return (total + arrived.astype(F32)).astype(BF16)

    right = shift(step_sum(4), "z", NZ, 1)
    left = shift(step_sum(-3), "z", NZ, -1)
    for n in (3, 2, 1):
        right = shift(step_sum(n, right), "z", NZ, 1)
        if n > 1:
            left = shift(step_sum(1 - n, left), "z", NZ, -1)
    back_block = own[:128].astype(F32) + theirs[:128].astype(F32)
    back_block = back_block + right.astype(F32) + left.astype(F32)
    input_grad = (back_block * dot(hot[:128], r3)).astype(BF16)

    out_term, scaled_in = jnp.zeros((16, 1024), F32), []
    for n, first in enumerate((0, NEAR)):
        parts = held[2 * n : 2 * n + 2]
        scaled, out_term = call(
            functools.partial(front_kernel, first),
            [((parts[0].shape[0] * 2, 1024), BF16), term], 10,
            hot, hot_t, r3, weight, cot_all, *parts, out_term,
        )
        scaled_in.append(scaled)
    weight_grad = grad_part(*scaled_in, scaled_cot, 0)
    weight_grad = grad_part(*scaled_in, scaled_cot, 1, (weight_grad,))
    in_term, out_term = in_term[:8], out_term[:8]
    in_term = in_term + flip(in_term, "c", 2, 1)
    for bit in (1, 2, 4):
        in_term = in_term + flip(in_term, "z", NZ, bit)
    for axis, bit in (("x", 1), ("y", 1), ("x", 2), ("y", 2)):
        out_term = out_term + flip(out_term, axis, 4, bit)
    return (input_grad, weight_grad, in_term, out_term)


def solution(mesh):
    fine = Mesh(mesh.devices.reshape(NX, NY, NZ, 2), ("x", "y", "z", "c"))
    row, col = ("x", "y"), ("z", "c")
    return jax.shard_map(
        step,
        mesh=fine,
        in_specs=(P(col, row), P(row, col), P(row, col), P(None, row), P(None, col), P()),
        out_specs=(P(col, row), P(row, col), P(None, row), P(None, col)),
        check_vma=False,
    )
```
